32 devices in a mesh: traj: 8 (over z, core), amp: 4 (over y, x).
Axes of the slice: x: 2, y: 2, z: 4, core: 2. Of those that a mesh axis runs over, the one named last changes fastest.
Arguments:
- amplitudes: float32 [8, 2, 524288], P('traj', None, 'amp'), parts along dimension 0, may hold values from -6 to 6
- couplings: float32 [18], replicated, may hold values from 0.5 to 2
- fields: float32 [19], replicated, may hold values from 0.5 to 2
- decays: float32 [19], replicated, may hold values from 0.2 to 2
- channel: int32 [8], P('traj'), parts along dimension 0, may hold values from 0 to 19
Outputs:
- evolved_state: float32 [8, 2, 524288], P('traj', None, 'amp'), parts along dimension 0
The draws below stay inside these ranges and needn't reach their ends.
There are 8 independent parts, one for each index of `traj`. The reference program is written for one: setup_inputs(seed, part) draws one part's arguments, and reference() takes and returns one part's arrays. A program takes and returns all parts, laid end to end along the dimension named above; an argument that names none is the same for every part. Nothing has to cross between parts.
Inputs may be any that keep to these rules, and one draw needn't show every extreme that they name: `channel`: the value 19 means that the trajectory does not jump.
All inputs are finite; a program needn't handle non-finite values.
Results may differ from the reference program's by a relative error of at most 0.0003.
Values sent between devices are 32-bit elements; how exact they have to be, the bound alone decides.
No kernel may reach another device: no remote copies, remote signals or barrier semaphores. Data moves between devices by JAX's collectives and lax.ppermute only.
A program may use at most 256 MiB of HBM per device.

```python
import math
import jax
import jax.numpy as jnp
from jax import lax

SPINS = 19
KRYLOV = 8
TRAJ = 1
AMPS = 524288


def steps_of(rng, dims, cuts, smallest, largest):
    def one(dim, shards_of):
        steps = jax.random.uniform(jax.random.fold_in(jax.random.fold_in(rng, 6), dim), (shards_of,), jnp.float32, smallest / len(cuts), largest / len(cuts))
        return jnp.repeat(jnp.exp(steps), dims[dim] // shards_of).reshape((-1,) + (1,) * (len(dims) - dim - 1))

    factor_of = one(*cuts[0])
    for cut in cuts[1:]:
        factor_of = factor_of * one(*cut)
    return factor_of


def noise(stream_key, dims, deviation, most, pieces=(), kind=jnp.bfloat16):
    drawn = jax.random.normal(stream_key, dims, jnp.float32) * deviation
    if len(pieces) > 0:
        drawn = steps_of(stream_key, dims, pieces, -0.22, 0.18) * drawn
    return jnp.clip(drawn, min=-most, max=most).astype(kind)


def setup_inputs(seed: int = 0, part: int = 0) -> dict:
    streams_of = jax.random.split(jax.random.key(seed), 6)
    own_keys = jax.random.split(jax.random.fold_in(streams_of[5], part), 6)
    amplitudes = noise(own_keys[0], (TRAJ, 2, AMPS), 1.0, 6.0, ((2, 4),), jnp.float32)
    couplings = jnp.clip(jnp.exp(jax.random.uniform(streams_of[1], (SPINS - 1,), jnp.float32, math.log(0.5), math.log(2.0))), 0.5, 2.0)
    fields = jnp.clip(jnp.exp(jax.random.uniform(streams_of[2], (SPINS,), jnp.float32, math.log(0.5), math.log(2.0))), 0.5, 2.0)
    decays = jnp.clip(jnp.exp(jax.random.uniform(streams_of[3], (SPINS,), jnp.float32, math.log(0.2), math.log(2.0))), 0.2, 2.0)
    channel = jax.random.randint(own_keys[4], (TRAJ,), 0, SPINS + 1).astype(jnp.int32)
    return dict(amplitudes=amplitudes, couplings=couplings, fields=fields, decays=decays, channel=channel)


time_step = 0.7
squarings = 8
taylor_order = 10
highest = lax.Precision.HIGHEST

def flip_spin(vector, spin_pos):
    leading = vector.shape[:-1]
    length = vector.shape[-1]
    parted = vector.reshape(leading + (length >> spin_pos + 1, 2, 1 << spin_pos))
    return jnp.flip(parted, axis=len(leading) + 1).reshape(vector.shape)

def apply_heff(vector, fields, diag_real, diag_imag):
    flipped = jnp.zeros_like(vector)
    for spin_pos in range(SPINS):
        flipped = flipped + fields[spin_pos] * flip_spin(vector, spin_pos)
    real_part = vector[:, 0]
    imag_part = vector[:, 1]
    out_real = diag_real * real_part - diag_imag * imag_part - flipped[:, 0]
    out_imag = diag_real * imag_part + diag_imag * real_part - flipped[:, 1]
    return jnp.stack([out_real, out_imag], axis=1)

def krylov_weights(scale_norm, hess_real, hess_imag):
    a_real = time_step * hess_imag
    a_imag = -time_step * hess_real
    upper_half = jnp.concatenate([a_real, -a_imag], axis=2)
    lower_half = jnp.concatenate([a_imag, a_real], axis=2)
    scaled = jnp.concatenate([upper_half, lower_half], axis=1) / 2.0 ** squarings
    identity = jnp.broadcast_to(jnp.eye(2 * KRYLOV, dtype=jnp.float32), scaled.shape)
    series = identity
    for degree in range(taylor_order, 0, -1):
        series = identity + jnp.einsum('tij,tjk->tik', scaled, series, precision=highest) / degree
    for repeat in range(squarings):
        series = jnp.einsum('tij,tjk->tik', series, series, precision=highest)
    first_column = series[:, :, 0] * scale_norm[:, None]
    return (first_column[:, :KRYLOV], first_column[:, KRYLOV:])

def reference(amplitudes, couplings, fields, decays, channel):
    traj_count = amplitudes.shape[0]
    position = jnp.arange(AMPS, dtype=jnp.int32)
    occupation = [(position >> spin_pos & 1).astype(jnp.float32) for spin_pos in range(SPINS)]
    diag_real = jnp.zeros((AMPS,), jnp.float32)
    for spin_pos in range(SPINS - 1):
        diag_real = diag_real - couplings[spin_pos] * (1.0 - 2.0 * occupation[spin_pos]) * (1.0 - 2.0 * occupation[spin_pos + 1])
    diag_imag = jnp.zeros((AMPS,), jnp.float32)
    for spin_pos in range(SPINS):
        diag_imag = diag_imag - 0.5 * decays[spin_pos] * occupation[spin_pos]
    scale_norm = jnp.sqrt(lax.optimization_barrier(jnp.sum(amplitudes * amplitudes, axis=(1, 2))))
    krylov_basis = [amplitudes / scale_norm[:, None, None]]
    hess_real = jnp.zeros((traj_count, KRYLOV, KRYLOV), jnp.float32)
    hess_imag = jnp.zeros((traj_count, KRYLOV, KRYLOV), jnp.float32)
    for column in range(KRYLOV):
        applied = apply_heff(krylov_basis[column], fields, diag_real, diag_imag)
        stacked = jnp.stack(krylov_basis, axis=1)
        swapped = jnp.stack([applied[:, 1], -applied[:, 0]], axis=1)
        proj_real = jnp.einsum('tkca,tca->tk', stacked, applied, precision=highest)
        proj_imag = jnp.einsum('tkca,tca->tk', stacked, swapped, precision=highest)
        hess_real = hess_real.at[:, :column + 1, column].set(proj_real)
        hess_imag = hess_imag.at[:, :column + 1, column].set(proj_imag)
        if column + 1 < KRYLOV:
            comb_real = jnp.einsum('tk,tka->ta', proj_real, stacked[:, :, 0], precision=highest) - jnp.einsum('tk,tka->ta', proj_imag, stacked[:, :, 1], precision=highest)
            comb_imag = jnp.einsum('tk,tka->ta', proj_real, stacked[:, :, 1], precision=highest) + jnp.einsum('tk,tka->ta', proj_imag, stacked[:, :, 0], precision=highest)
            residual = applied - jnp.stack([comb_real, comb_imag], axis=1)
            column_norm = jnp.sqrt(lax.optimization_barrier(jnp.sum(residual * residual, axis=(1, 2))))
            hess_real = hess_real.at[:, column + 1, column].set(column_norm)
            krylov_basis.append(residual / column_norm[:, None, None])
    weights_real, weights_imag = krylov_weights(scale_norm, hess_real, hess_imag)
    stacked = jnp.stack(krylov_basis, axis=1)
    new_real = jnp.einsum('tk,tka->ta', weights_real, stacked[:, :, 0], precision=highest) - jnp.einsum('tk,tka->ta', weights_imag, stacked[:, :, 1], precision=highest)
    new_imag = jnp.einsum('tk,tka->ta', weights_real, stacked[:, :, 1], precision=highest) + jnp.einsum('tk,tka->ta', weights_imag, stacked[:, :, 0], precision=highest)
    propagated = jnp.stack([new_real, new_imag], axis=1)
    lowered = jnp.zeros_like(propagated)
    for spin_pos in range(SPINS):
        vacant = occupation[spin_pos] == 0.0
        lowered_term = jnp.where(vacant[None, None, :], flip_spin(propagated, spin_pos), 0.0)
        lowered = jnp.where((channel == spin_pos)[:, None, None], lowered_term, lowered)
    jumped = channel < SPINS
    squared_sum = jnp.where(jumped, lax.optimization_barrier(jnp.sum(lowered * lowered, axis=(1, 2))), jnp.float32(AMPS))
    lowered = lowered * jnp.sqrt(AMPS / squared_sum)[:, None, None]
    return jnp.where(jumped[:, None, None], lowered, propagated)
```

```python
import functools
import jax
import jax.numpy as jnp
from jax import lax
from jax.experimental import pallas as pl
from jax.experimental.pallas import tpu as pltpu
from jax.sharding import PartitionSpec as P

KRYLOV = 8
time_step = 0.7
squarings = 8
taylor_order = 10
highest = lax.Precision.HIGHEST
LANES = 128
TILE = (8, LANES)
BLOCK = 256
CHUNK = 2 * BLOCK


def partner(value, mask):
    count = lax.axis_size("amp")
    return lax.ppermute(value, "amp", [(i, i ^ mask) for i in range(count)])


def gather_state(own, high_bits):
    rows = own.shape[2] // LANES
    if high_bits == 2:
        half = own.shape[2] // 2
        first = partner(own, 1)
        second = partner(own, 2)
        third_low = partner(first[:, :, :half], 2)
        third_high = partner(second[:, :, half:], 1)
        return [
            (0, own),
            (rows, first),
            (2 * rows, second),
            (3 * rows, third_low),
            (3 * rows + rows // 2, third_high),
        ]
    pieces = [(0, own)]
    for bit in range(high_bits):
        pieces += [(start + (rows << bit), partner(piece, 1 << bit)) for start, piece in pieces]
    return pieces


def interleaved(piece):
    rows = piece.shape[2] // LANES
    return piece.reshape(2, rows, LANES).transpose(1, 0, 2).reshape(2 * rows, LANES)


def splat(value):
    return jnp.broadcast_to(value, TILE)


def total(acc):
    return splat(jnp.sum(acc, keepdims=True))


def cmul(a, b):
    return (a[0] * b[0] - a[1] * b[1], a[0] * b[1] + a[1] * b[0])


def conj(a):
    return (a[0], -a[1])


def sub(a, b):
    return (a[0] - b[0], a[1] - b[1])


def scale(a, r):
    return (a[0] * r, a[1] * r)


def kernel(spins, starts, *refs):
    count = len(starts)
    fields, row_real, row_imag, channel, device = refs[:5]
    low_real, low_imag, mats = refs[5:8]
    pieces = refs[8 : 8 + count]
    out = refs[8 + count]
    basis_r, basis_i, high, low, table = refs[9 + count :]
    rows_total = basis_r.shape[1]
    groups = rows_total // 8
    rows_out = out.shape[0] // 2
    zero = jnp.zeros(TILE, jnp.float32)

    norm = zero
    for start, piece in zip(starts, pieces):

        def take(g, acc, start=start, piece=piece):
            re = piece[pl.ds(pl.multiple_of(g * 16, 16), 8, stride=2), :]
            im = piece[pl.ds(g * 16 + 1, 8, stride=2), :]
            row = pl.multiple_of(start + g * 8, 8)
            basis_r[0, pl.ds(row, 8), :] = re
            basis_i[0, pl.ds(row, 8), :] = im
            return acc + (re * re + im * im)

        norm = lax.fori_loop(0, piece.shape[0] // 16, take, norm, unroll=8)

    def product(part, block, slot, row):
        xh = high[2 * part + block]
        xl = low[2 * part + block]
        return xh, xl

    def chunk_flips(c, slot):
        left_h, left_l, right_h, right_l = mats[0], mats[1], mats[2], mats[3]
        base = pl.multiple_of(c * CHUNK, CHUNK)
        for part, ref in ((0, basis_r), (1, basis_i)):
            xh, xl = high[part], low[part]
            dot = functools.partial(jnp.dot, preferred_element_type=jnp.float32)
            y = dot(left_h, xh) + dot(left_l, xh) + dot(left_h, xl)
            y = y + dot(xh, right_h) + dot(xh, right_l) + dot(xl, right_h)
            ref[slot, pl.ds(base, BLOCK), :] = y[:, :LANES]
            ref[slot, pl.ds(base + BLOCK, BLOCK), :] = y[:, LANES:]

    def halves(part, block, r, value):
        h = value.astype(jnp.bfloat16)
        l = (value - h.astype(jnp.float32)).astype(jnp.bfloat16)
        high[part, pl.ds(r, 16), pl.ds(block * LANES, LANES)] = h
        low[part, pl.ds(r, 16), pl.ds(block * LANES, LANES)] = l

    gram = {}
    diag_a, real_b, norms = [], [], [total(norm)]
    gram[0, 0] = (norms[0], zero)
    inner = None
    scale0 = lax.rsqrt(norms[0])
    for step in range(KRYLOV):
        def make(c, acc, step=step):
            base = pl.multiple_of(c * CHUNK, CHUNK)
            for block in range(2):
                for r in range(0, BLOCK, 16):
                    at = pl.ds(base + block * BLOCK + r, 16)
                    re = basis_r[step, at, :]
                    im = basis_i[step, at, :]
                    if step > 0:
                        pr, pi = basis_r[step - 1, at, :], basis_i[step - 1, at, :]
                        ar = jnp.concatenate([diag_a[step - 1][0]] * 2)
                        ai = jnp.concatenate([diag_a[step - 1][1]] * 2)
                        if step == 1:
                            s = jnp.concatenate([scale0] * 2)
                            re, im = re * s, im * s
                        re = re - (ar * pr - ai * pi)
                        im = im - (ar * pi + ai * pr)
                        if step > 1:
                            b = jnp.concatenate([real_b[step - 1]] * 2)
                            re = re - b * basis_r[step - 2, at, :]
                            im = im - b * basis_i[step - 2, at, :]
                        basis_r[step, at, :] = re
                        basis_i[step, at, :] = im
                        sq = re * re + im * im
                        acc = acc + (sq[:8] + sq[8:])
                    halves(0, block, r, re)
                    halves(1, block, r, im)
            chunk_flips(c, step + 1)
            return acc

        square = lax.fori_loop(0, rows_total // CHUNK, make, zero)
        if step > 0:
            square = total(square)
            gram[step, step] = (square, zero)
            norms.append(square)

        far = [(b, fields[7 + b]) for b in range(9, spins - 7)]
        lr, li = (low_real[0], low_real[1]), low_imag[...]

        def apply(c, accs, step=step):
            accs = list(accs)
            base = pl.multiple_of(c * 64, 64)
            for r in range(8):
                at = pl.ds(pl.multiple_of(base + 8 * r, 8), 8)
                xr, xi = basis_r[step, at, :], basis_i[step, at, :]
                wr, wi = basis_r[step + 1, at, :], basis_i[step + 1, at, :]
                for bit, weight in far:
                    other = pl.ds(pl.multiple_of((base ^ (1 << bit)) + 8 * r, 8), 8)
                    wr = wr - weight * basis_r[step, other, :]
                    wi = wi - weight * basis_i[step, other, :]
                dr = lr[r & 1] + row_real[c * 8 + r]
                di = li + row_imag[c * 8 + r]
                wr = wr + (dr * xr - di * xi)
                wi = wi + (dr * xi + di * xr)
                if step + 1 < KRYLOV:
                    basis_r[step + 1, at, :] = wr
                    basis_i[step + 1, at, :] = wi
                for k in range(step + 1):
                    ur, ui = (xr, xi) if k == step else (basis_r[k, at, :], basis_i[k, at, :])
                    accs[2 * k] = accs[2 * k] + (ur * wr + ui * wi)
                    accs[2 * k + 1] = accs[2 * k + 1] + (ur * wi - ui * wr)
            return tuple(accs)

        sums = lax.fori_loop(0, groups // 8, apply, (zero,) * (2 * step + 2))
        inner = [(total(sums[2 * k]), total(sums[2 * k + 1])) for k in range(step + 1)]
        inverse = 1.0 / norms[step]
        unit = scale0 if step == 0 else jnp.ones(TILE, jnp.float32)
        inner = [scale(x, unit) for x in inner] if step == 0 else inner
        diag_a.append(scale(inner[step], inverse))
        real_b.append(inner[step - 1][0] / norms[step - 1] if step > 0 else zero)
        if step + 1 < KRYLOV:
            for k in range(step + 1):
                g = lambda i, j: gram[i, j] if i <= j else conj(gram[j, i])
                value = sub(inner[k], cmul(diag_a[step], g(k, step)))
                if step > 0:
                    value = sub(value, scale(g(k, step - 1), real_b[step]))
                gram[k, step + 1] = value

    size = [jnp.sqrt(x) for x in norms]
    inv = [1.0 / x for x in size]
    mat = {}
    for j in range(KRYLOV):
        for k in range(j + 1):
            mat[j, k] = conj(scale(gram[k, j], inv[k] * inv[j]))
    rhs = [scale(inner[k], inv[k] * inv[KRYLOV - 1]) for k in range(KRYLOV)]
    factor, pivot = {}, []
    for j in range(KRYLOV):
        d = mat[j, j][0]
        for k in range(j):
            d = d - (factor[j, k][0] * factor[j, k][0] + factor[j, k][1] * factor[j, k][1]) * pivot[k]
        pivot.append(d)
        r = 1.0 / d
        for i in range(j + 1, KRYLOV):
            x = mat[i, j]
            for k in range(j):
                x = sub(x, scale(cmul(factor[i, k], conj(factor[j, k])), pivot[k]))
            factor[i, j] = scale(x, r)
    last = list(rhs)
    for i in range(KRYLOV):
        for k in range(i):
            last[i] = sub(last[i], cmul(factor[i, k], last[k]))
    last = [scale(x, 1.0 / pivot[i]) for i, x in enumerate(last)]
    for i in reversed(range(KRYLOV)):
        for k in range(i + 1, KRYLOV):
            last[i] = sub(last[i], cmul(conj(factor[k, i]), last[k]))

    entries = {}
    for j in range(KRYLOV - 1):
        entries[j, j] = diag_a[j] if j > 0 else scale(diag_a[0], size[0])
        grow = size[1] if j == 0 else size[j + 1] * inv[j]
        entries[j + 1, j] = (grow, zero)
        if j > 0:
            entries[j - 1, j] = (real_b[j] * (size[j - 1] * inv[j]), zero)
    for i in range(KRYLOV):
        entries[i, KRYLOV - 1] = last[i]
    order = 2 * KRYLOV
    row_id = lax.broadcasted_iota(jnp.int32, (LANES, LANES), 0)
    col_id = lax.broadcasted_iota(jnp.int32, (LANES, LANES), 1)
    code = lax.broadcasted_iota(jnp.int32, TILE, 0) * LANES + lax.broadcasted_iota(jnp.int32, TILE, 1)
    quads = [[zero, zero], [zero, zero]]
    for (i, j), (re, im) in entries.items():
        here = code == i * LANES + j
        there = code == i * LANES + j + KRYLOV
        ar, ai = time_step * im, -time_step * re
        quads[0][0] = jnp.where(here, ar, jnp.where(there, -ai, quads[0][0]))
        quads[1][0] = jnp.where(here, ai, jnp.where(there, ar, quads[1][0]))
    table[...] = jnp.zeros_like(table)
    table[0:8, :] = quads[0][0] * (1.0 / 2.0**squarings)
    table[8:16, :] = quads[1][0] * (1.0 / 2.0**squarings)
    one = table[...]
    eye = jnp.where((row_id == col_id) & (row_id < order), 1.0, 0.0)
    times = functools.partial(jnp.dot, precision=highest, preferred_element_type=jnp.float32)
    two = times(one, one)
    three = times(two, one)
    f = [1.0]
    for d in range(1, taylor_order + 1):
        f.append(f[-1] / d)
    series = f[9] * eye + f[10] * one
    for d in (6, 3, 0):
        series = (f[d] * eye + f[d + 1] * one + f[d + 2] * two) + times(three, series)
    for repeat in range(squarings):
        series = times(series, series)
    table[...] = series
    weights = []
    for k in range(KRYLOV):
        c = size[0] * inv[k]
        weights.append((splat(table[k : k + 1, 0:1]) * c, splat(table[k + 8 : k + 9, 0:1]) * c))

    jump = channel[0]
    first = device[0]
    lane = lax.broadcasted_iota(jnp.int32, TILE, 1)
    sublane = lax.broadcasted_iota(jnp.int32, TILE, 0)
    inside = sublane * LANES + lane
    far_jump = jump >= 10
    low_bit = jnp.where(far_jump, 0, jump)
    high_bit = jnp.where(far_jump, jump - 10, 0)
    set_low = ((inside >> low_bit) & 1) == 1
    groups_out = rows_out // 8
    absolute = first * groups_out

    def combine(c, acc):
        for r in range(4):
            g = c * 4 + r
            at = pl.ds(pl.multiple_of(g * 8, 8), 8)
            pr, pi = zero, zero
            for k in range(KRYLOV):
                cr, ci = weights[k]
                ur, ui = basis_r[k, at, :], basis_i[k, at, :]
                pr = pr + (cr * ur - ci * ui)
                pi = pi + (cr * ui + ci * ur)
            basis_r[KRYLOV, at, :] = pr
            basis_i[KRYLOV, at, :] = pi
            raised = jnp.where(far_jump, ((g ^ absolute) >> high_bit) & 1, 1)
            acc = acc + raised.astype(jnp.float32) * (pr * pr + pi * pi)
        return acc

    weight = lax.fori_loop(0, groups // 4, combine, zero)
    weight = total(jnp.where(set_low | far_jump, weight, 0.0))
    gain = jnp.sqrt((rows_total * LANES) / weight)

    def put(g, re, im):
        out[pl.ds(pl.multiple_of(g * 16, 16), 8, stride=2), :] = re
        out[pl.ds(g * 16 + 1, 8, stride=2), :] = im

    def stay(g, _):
        at = pl.ds(pl.multiple_of(g * 8, 8), 8)
        put(g, basis_r[KRYLOV, at, :], basis_i[KRYLOV, at, :])
        return 0

    def lower_far(g, _):
        at = pl.ds(pl.multiple_of((g ^ (1 << high_bit)) * 8, 8), 8)
        vacant = 1 - (((g ^ absolute) >> high_bit) & 1)
        factor = gain * vacant.astype(jnp.float32)
        put(g, factor * basis_r[KRYLOV, at, :], factor * basis_i[KRYLOV, at, :])
        return 0

    def lower_lane(g, _):
        at = pl.ds(pl.multiple_of(g * 8, 8), 8)
        shift = LANES - (1 << low_bit)
        factor = jnp.where(set_low, 0.0, gain)
        put(
            g,
            factor * pltpu.roll(basis_r[KRYLOV, at, :], shift, 1),
            factor * pltpu.roll(basis_i[KRYLOV, at, :], shift, 1),
        )
        return 0

    def lower_sublane(bit):
        def run(g, _):
            at = pl.ds(pl.multiple_of(g * 8, 8), 8)
            shift = 8 - (1 << bit)
            factor = jnp.where(set_low, 0.0, gain)
            put(
                g,
                factor * pltpu.roll(basis_r[KRYLOV, at, :], shift, 0),
                factor * pltpu.roll(basis_i[KRYLOV, at, :], shift, 0),
            )
            return 0

        return run

    def over_output(run):
        lax.fori_loop(0, groups_out, run, 0, unroll=4)

    pl.when(jump == spins)(lambda: over_output(stay))
    pl.when((jump >= 10) & (jump < spins))(lambda: over_output(lower_far))
    pl.when(jump < 7)(lambda: over_output(lower_lane))
    for bit in range(3):
        pl.when(jump == 7 + bit)(functools.partial(over_output, lower_sublane(bit)))


def body(amplitudes, couplings, fields, decays, channel):
    node_count = lax.axis_size("amp")
    high_bits = node_count.bit_length() - 1
    device = lax.axis_index("amp")
    local_len = amplitudes.shape[2]
    spins = fields.shape[0]
    rows_total = node_count * local_len // LANES
    groups = rows_total // 8
    pieces = gather_state(amplitudes, high_bits)

    tile_ids = jnp.arange(8 * LANES, dtype=jnp.int32).reshape(TILE)
    group_ids = jnp.arange(groups, dtype=jnp.int32) ^ (device * (local_len // LANES // 8))
    bits_low = [(tile_ids >> i & 1).astype(jnp.float32) for i in range(10)]
    bits_row = [(group_ids >> i & 1).astype(jnp.float32) for i in range(spins - 10)]
    z_low = [1.0 - 2.0 * b for b in bits_low]
    z_row = [1.0 - 2.0 * b for b in bits_row]
    low_real = -sum(couplings[i] * z_low[i] * z_low[i + 1] for i in range(9))
    low_real = jnp.stack([low_real - couplings[9] * z_low[9], low_real + couplings[9] * z_low[9]])
    low_imag = -0.5 * sum(decays[i] * bits_low[i] for i in range(10))
    row_real = -sum(couplings[10 + i] * z_row[i] * z_row[i + 1] for i in range(spins - 11))
    row_imag = -0.5 * sum(decays[10 + i] * bits_row[i] for i in range(spins - 10))
    ids = jnp.arange(BLOCK, dtype=jnp.int32)
    crossed = ids[:, None] ^ ids[None, :]
    left = -sum(fields[7 + i] * (crossed == 1 << i).astype(jnp.float32) for i in range(8))
    right = -sum(
        fields[i if i < 7 else 15] * (crossed == 1 << i).astype(jnp.float32) for i in range(8)
    )

    def split(m):
        h = lax.reduce_precision(m, 8, 7)
        return [h.astype(jnp.bfloat16), (m - h).astype(jnp.bfloat16)]

    mats = jnp.stack(split(left) + split(right))
    smem = pl.BlockSpec(memory_space=pltpu.SMEM)
    vmem = pl.BlockSpec(memory_space=pltpu.VMEM)
    result = pl.pallas_call(
        functools.partial(kernel, spins, [start for start, _ in pieces]),
        out_shape=jax.ShapeDtypeStruct((2 * local_len // LANES, LANES), jnp.float32),
        in_specs=[smem] * 5 + [vmem] * (3 + len(pieces)),
        out_specs=vmem,
        scratch_shapes=[
            pltpu.VMEM((KRYLOV + 1, rows_total, LANES), jnp.float32),
            pltpu.VMEM((KRYLOV + 1, rows_total, LANES), jnp.float32),
            pltpu.VMEM((2, BLOCK, BLOCK), jnp.bfloat16),
            pltpu.VMEM((2, BLOCK, BLOCK), jnp.bfloat16),
            pltpu.VMEM((LANES, LANES), jnp.float32),
        ],
        compiler_params=pltpu.CompilerParams(vmem_limit_bytes=60 * 1024 * 1024),
        name="trajectory",
    )(
        fields,
        row_real,
        row_imag,
        channel.reshape(1),
        device.reshape(1).astype(jnp.int32),
        low_real,
        low_imag,
        mats,
        *[interleaved(piece) for _, piece in pieces],
    )
    rows = local_len // LANES
    return result.reshape(rows, 2, LANES).transpose(1, 0, 2).reshape(1, 2, local_len)


def solution(mesh):
    placed = (P("traj", None, "amp"), P(), P(), P(), P("traj"))
    return jax.shard_map(
        body, mesh=mesh, in_specs=placed, out_specs=P("traj", None, "amp"), check_vma=False
    )
```

```python
import functools
import jax
import jax.numpy as jnp
from jax import lax
from jax.experimental import pallas as pl
from jax.experimental.pallas import tpu as pltpu
from jax.sharding import PartitionSpec as P

KRYLOV = 8
time_step = 0.7
squarings = 8
taylor_order = 10
highest = lax.Precision.HIGHEST
LANES = 128
TILE = (8, LANES)
BLOCK = 256
CHUNK = 2 * BLOCK
SET_BITS = 2


def partner(value, mask):
    count = lax.axis_size("amp")
    return lax.ppermute(value, "amp", [(i, i ^ mask) for i in range(count)])


def gather_state(own, high_bits):
    rows = own.shape[2] // LANES
    if high_bits == 2:
        half = own.shape[2] // 2
        first = partner(own, 1)
        second = partner(own, 2)
        third_low = partner(first[:, :, :half], 2)
        third_high = partner(second[:, :, half:], 1)
        return [
            (0, own),
            (rows, first),
            (2 * rows, second),
            (3 * rows, third_low),
            (3 * rows + rows // 2, third_high),
        ]
    pieces = [(0, own)]
    for bit in range(high_bits):
        pieces += [(start + (rows << bit), partner(piece, 1 << bit)) for start, piece in pieces]
    return pieces


def interleaved(piece):
    rows = piece.shape[2] // LANES
    return piece.reshape(2, rows, LANES).transpose(1, 0, 2).reshape(2 * rows, LANES)


def splat(value):
    return jnp.broadcast_to(value, TILE)


def total(acc):
    return splat(jnp.sum(acc, keepdims=True))


def cmul(a, b):
    return (a[0] * b[0] - a[1] * b[1], a[0] * b[1] + a[1] * b[0])


def conj(a):
    return (a[0], -a[1])


def sub(a, b):
    return (a[0] - b[0], a[1] - b[1])


def scale(a, r):
    return (a[0] * r, a[1] * r)


def prepare(spins, couplings, fields, decays, device, mats, low, rows):
    tile_ids = lax.broadcasted_iota(jnp.int32, TILE, 0) * LANES + lax.broadcasted_iota(jnp.int32, TILE, 1)
    bits = [(tile_ids >> i & 1).astype(jnp.float32) for i in range(10)]
    signs = [1.0 - 2.0 * b for b in bits]
    real = -sum(couplings[i] * (signs[i] * signs[i + 1]) for i in range(9))
    bond = couplings[9] * signs[9]
    low[0:8, :] = real - bond
    low[8:16, :] = real + bond
    low[16:24, :] = -0.5 * sum(decays[i] * bits[i] for i in range(10))
    low[24:32, :] = jnp.zeros(TILE, jnp.float32)
    wide = rows.shape
    ids = lax.broadcasted_iota(jnp.int32, wide, 1) ^ device[0]
    bits = [(ids >> i & 1).astype(jnp.float32) for i in range(spins - 10)]
    signs = [1.0 - 2.0 * b for b in bits]
    real = -sum(couplings[10 + i] * (signs[i] * signs[i + 1]) for i in range(spins - 11))
    imag = -0.5 * sum(decays[10 + i] * bits[i] for i in range(spins - 10))
    rows[...] = jnp.where(lax.broadcasted_iota(jnp.int32, wide, 0) == 0, real, imag)
    for r in range(0, BLOCK, 32):
        shape = (32, BLOCK)
        crossed = (r + lax.broadcasted_iota(jnp.int32, shape, 0)) ^ lax.broadcasted_iota(jnp.int32, shape, 1)
        for side in range(2):
            m = jnp.zeros(shape, jnp.float32)
            for i in range(8):
                spin = 7 + i if side == 0 else (i if i < 7 else 15)
                m = jnp.where(crossed == 1 << i, -fields[spin], m)
            h = m.astype(jnp.bfloat16)
            mats[2 * side, r : r + 32, :] = h
            mats[2 * side + 1, r : r + 32, :] = (m - h.astype(jnp.float32)).astype(jnp.bfloat16)


def kernel(spins, starts, *refs):
    count = len(starts)
    fields, row_table, channel, device = refs[:4]
    low_table, mats = refs[4:6]
    pieces = refs[6 : 6 + count]
    out = refs[6 + count]
    basis_r, basis_i, cur_r, cur_i, new_r, new_i, high, low, table, coefs, norms, inner_r, inner_i = refs[7 + count :]
    rows_total = new_r.shape[0]
    groups = rows_total // 8
    rows_out = out.shape[0] // 2
    zero = jnp.zeros(TILE, jnp.float32)
    dot = functools.partial(jnp.dot, preferred_element_type=jnp.float32)

    for start, piece in zip(starts, pieces):

        def take(g, carry, start=start, piece=piece):
            row = pl.multiple_of(start + g * 8, 8)
            new_r[pl.ds(row, 8), :] = piece[pl.ds(pl.multiple_of(g * 16, 16), 8, stride=2), :]
            new_i[pl.ds(row, 8), :] = piece[pl.ds(g * 16 + 1, 8, stride=2), :]
            return carry

        lax.fori_loop(0, piece.shape[0] // 16, take, 0, unroll=8)

    def block_flips(c):
        base = pl.multiple_of(c * CHUNK, CHUNK)
        for part, ref in ((0, new_r), (1, new_i)):
            xh, xl = high[part, c], low[part, c]
            y = dot(mats[0], xh) + dot(mats[1], xh) + dot(mats[0], xl)
            y = y + dot(xh, mats[2]) + dot(xh, mats[3]) + dot(xl, mats[2])
            ref[pl.ds(base, BLOCK), :] = y[:, :LANES]
            ref[pl.ds(base + BLOCK, BLOCK), :] = y[:, LANES:]

    def halves(part, c, block, r, value):
        h = value.astype(jnp.bfloat16)
        l = (value - h.astype(jnp.float32)).astype(jnp.bfloat16)
        high[part, c, pl.ds(r, 16), pl.ds(block * LANES, LANES)] = h
        low[part, c, pl.ds(r, 16), pl.ds(block * LANES, LANES)] = l

    near = [(b, fields[7 + b]) for b in range(9, 9 + SET_BITS)]
    far = [(b, fields[7 + b]) for b in range(9 + SET_BITS, spins - 7)]
    sets = 1 << SET_BITS
    span = CHUNK * sets
    ones = jnp.ones(TILE, jnp.float32)
    for i, value in enumerate((ones, zero, zero, zero)):
        coefs[i] = value

    def clear(t, carry):
        at = pl.ds(pl.multiple_of(t * 8, 8), 8)
        for ref in (cur_r, cur_i, basis_r.at[0], basis_i.at[0]):
            ref[at, :] = zero
        return carry

    lax.fori_loop(0, groups, clear, 0, unroll=8)

    def one_step(step):
        earlier = jnp.maximum(step - 2, 0)

        def make(t, acc):
            start = pl.multiple_of(t * span, span)
            sc, ar, ai, b = [jnp.concatenate([coefs[i], coefs[i]]) for i in range(4)]
            lr, li = (low_table[0:8, :], low_table[8:16, :]), low_table[16:24, :]

            def vector(i, acc):
                for block in range(2):
                    for r in range(0, BLOCK, 16):
                        at = pl.ds(start + i * CHUNK + block * BLOCK + r, 16)
                        pr, pi = cur_r[at, :], cur_i[at, :]
                        re = sc * new_r[at, :] - (ar * pr - ai * pi) - b * basis_r[earlier, at, :]
                        im = sc * new_i[at, :] - (ar * pi + ai * pr) - b * basis_i[earlier, at, :]
                        cur_r[at, :] = re
                        cur_i[at, :] = im
                        sq = re * re + im * im
                        acc = acc + (sq[:8] + sq[8:])
                        c = t * sets + i
                        halves(0, c, block, r, re)
                        halves(1, c, block, r, im)
                return acc

            def rest(i):
                for r in range(0, CHUNK, 8):
                    row = i * CHUNK + r
                    at = pl.ds(start + row, 8)
                    xr, xi = cur_r[at, :], cur_i[at, :]
                    wr, wi = new_r[at, :], new_i[at, :]
                    g = t * (span // 8) + row // 8
                    dr = lr[(r // 8) & 1] + row_table[0, g]
                    di = li + row_table[1, g]
                    wr = wr + (dr * xr - di * xi)
                    wi = wi + (dr * xi + di * xr)
                    for bit, weight in near:
                        other = pl.ds(start + (row ^ (1 << bit)), 8)
                        wr = wr - weight * cur_r[other, :]
                        wi = wi - weight * cur_i[other, :]
                    new_r[at, :] = wr
                    new_i[at, :] = wi

            for i in range(sets):
                acc = vector(i, acc)
                block_flips(t * sets + i)
            for i in range(sets):
                rest(i)
            return acc

        norms[step] = total(lax.fori_loop(0, rows_total // span, make, zero))

    def products(step):
        count_rows = 32 if step < 2 else 16 if step < 5 else 8

        def apply(t, accs):
            base = pl.multiple_of(t * (8 * count_rows), 8 * count_rows)
            at = [pl.ds(pl.multiple_of(base + 8 * r, 8), 8) for r in range(count_rows)]
            w = []
            for r in range(count_rows):
                wr, wi = new_r[at[r], :], new_i[at[r], :]
                for bit, weight in far:
                    other = pl.ds(pl.multiple_of((base ^ (1 << bit)) + 8 * r, 8), 8)
                    wr = wr - weight * cur_r[other, :]
                    wi = wi - weight * cur_i[other, :]
                if step + 1 < KRYLOV:
                    new_r[at[r], :] = wr
                    new_i[at[r], :] = wi
                w.append((wr, wi))
            accs = list(accs)
            for k in range(step + 1):
                re, im = [], []
                for r in range(count_rows):
                    if k == step:
                        ur, ui = cur_r[at[r], :], cur_i[at[r], :]
                        basis_r[k, at[r], :] = ur
                        basis_i[k, at[r], :] = ui
                    else:
                        ur, ui = basis_r[k, at[r], :], basis_i[k, at[r], :]
                    wr, wi = w[r]
                    re.append(ur * wr + ui * wi)
                    im.append(ur * wi - ui * wr)
                    if len(re) == 4:
                        accs[2 * k] = accs[2 * k] + ((re[0] + re[1]) + (re[2] + re[3]))
                        accs[2 * k + 1] = accs[2 * k + 1] + ((im[0] + im[1]) + (im[2] + im[3]))
                        re, im = [], []
            return tuple(accs)

        sums = lax.fori_loop(0, groups // count_rows, apply, (zero,) * (2 * step + 2))
        unit = lax.rsqrt(norms[0]) if step == 0 else ones
        found = [total(x) * unit for x in sums]
        for k in range(step + 1):
            inner_r[step * KRYLOV + k] = found[2 * k]
            inner_i[step * KRYLOV + k] = found[2 * k + 1]
        inverse = 1.0 / norms[step]
        coefs[0] = unit
        coefs[1] = found[2 * step] * inverse
        coefs[2] = found[2 * step + 1] * inverse
        coefs[3] = found[2 * step - 2] / norms[step - 1] if step > 0 else zero

    @pl.loop(0, KRYLOV)
    def _(step):
        one_step(step)
        for s in range(KRYLOV):
            pl.when(step == s)(functools.partial(products, s))

    norm = [norms[j] for j in range(KRYLOV)]
    gram, diag_a, real_b = {(0, 0): (norm[0], zero)}, [], []
    read = lambda k, j: (inner_r[j * KRYLOV + k], inner_i[j * KRYLOV + k])
    g = lambda i, j: gram[i, j] if i <= j else conj(gram[j, i])
    for j in range(KRYLOV - 1):
        diag_a.append(scale(read(j, j), 1.0 / norm[j]))
        real_b.append(read(j - 1, j)[0] / norm[j - 1] if j > 0 else zero)
        for k in range(j + 1):
            value = sub(read(k, j), cmul(diag_a[j], g(k, j)))
            if j > 0:
                value = sub(value, scale(g(k, j - 1), real_b[j]))
            gram[k, j + 1] = value
        gram[j + 1, j + 1] = (norm[j + 1], zero)
    inner = [read(k, KRYLOV - 1) for k in range(KRYLOV)]

    size = [jnp.sqrt(x) for x in norm]
    inv = [1.0 / x for x in size]
    mat = {}
    for j in range(KRYLOV):
        for k in range(j + 1):
            mat[j, k] = conj(scale(gram[k, j], inv[k] * inv[j]))
    rhs = [scale(inner[k], inv[k] * inv[KRYLOV - 1]) for k in range(KRYLOV)]
    factor, pivot = {}, []
    for j in range(KRYLOV):
        d = mat[j, j][0]
        for k in range(j):
            d = d - (factor[j, k][0] * factor[j, k][0] + factor[j, k][1] * factor[j, k][1]) * pivot[k]
        pivot.append(d)
        r = 1.0 / d
        for i in range(j + 1, KRYLOV):
            x = mat[i, j]
            for k in range(j):
                x = sub(x, scale(cmul(factor[i, k], conj(factor[j, k])), pivot[k]))
            factor[i, j] = scale(x, r)
    last = list(rhs)
    for i in range(KRYLOV):
        for k in range(i):
            last[i] = sub(last[i], cmul(factor[i, k], last[k]))
    last = [scale(x, 1.0 / pivot[i]) for i, x in enumerate(last)]
    for i in reversed(range(KRYLOV)):
        for k in range(i + 1, KRYLOV):
            last[i] = sub(last[i], cmul(conj(factor[k, i]), last[k]))

    entries = {}
    for j in range(KRYLOV - 1):
        entries[j, j] = diag_a[j] if j > 0 else scale(diag_a[0], size[0])
        grow = size[1] if j == 0 else size[j + 1] * inv[j]
        entries[j + 1, j] = (grow, zero)
        if j > 0:
            entries[j - 1, j] = (real_b[j] * (size[j - 1] * inv[j]), zero)
    for i in range(KRYLOV):
        entries[i, KRYLOV - 1] = last[i]
    order = 2 * KRYLOV
    code = lax.broadcasted_iota(jnp.int32, TILE, 0) * LANES + lax.broadcasted_iota(jnp.int32, TILE, 1)
    quads = [[zero, zero], [zero, zero]]
    for (i, j), (re, im) in entries.items():
        here = code == i * LANES + j
        there = code == i * LANES + j + KRYLOV
        ar, ai = time_step * im, -time_step * re
        quads[0][0] = jnp.where(here, ar, jnp.where(there, -ai, quads[0][0]))
        quads[1][0] = jnp.where(here, ai, jnp.where(there, ar, quads[1][0]))
    table[...] = jnp.zeros_like(table)
    table[0:8, :] = quads[0][0] * (1.0 / 2.0**squarings)
    table[8:16, :] = quads[1][0] * (1.0 / 2.0**squarings)
    one = table[0:order, :]
    eye = jnp.where(
        lax.broadcasted_iota(jnp.int32, one.shape, 0) == lax.broadcasted_iota(jnp.int32, one.shape, 1), 1.0, 0.0
    )
    fill = jnp.zeros((LANES - order, LANES), jnp.float32)

    def times(a, b):
        return dot(a, jnp.concatenate([b, fill]), precision=highest)

    two = times(one, one)
    three = times(two, one)
    f = [1.0]
    for d in range(1, taylor_order + 1):
        f.append(f[-1] / d)
    series = f[9] * eye + f[10] * one
    for d in (6, 3, 0):
        series = (f[d] * eye + f[d + 1] * one + f[d + 2] * two) + times(three, series)
    for repeat in range(squarings):
        series = times(series, series)
    table[0:order, :] = series
    weights = []
    for k in range(KRYLOV):
        c = size[0] * inv[k]
        weights.append((splat(table[k : k + 1, 0:1]) * c, splat(table[k + 8 : k + 9, 0:1]) * c))

    jump = channel[0]
    first = device[0]
    lane = lax.broadcasted_iota(jnp.int32, TILE, 1)
    sublane = lax.broadcasted_iota(jnp.int32, TILE, 0)
    inside = sublane * LANES + lane
    far_jump = jump >= 10
    low_bit = jnp.where(far_jump, 0, jump)
    high_bit = jnp.where(far_jump, jump - 10, 0)
    set_low = ((inside >> low_bit) & 1) == 1
    groups_out = rows_out // 8
    absolute = first * groups_out

    def combine(c, acc):
        for r in range(4):
            g = c * 4 + r
            at = pl.ds(pl.multiple_of(g * 8, 8), 8)
            pr, pi = zero, zero
            for k in range(KRYLOV):
                cr, ci = weights[k]
                ur, ui = basis_r[k, at, :], basis_i[k, at, :]
                pr = pr + (cr * ur - ci * ui)
                pi = pi + (cr * ui + ci * ur)
            new_r[at, :] = pr
            new_i[at, :] = pi
            raised = jnp.where(far_jump, ((g ^ absolute) >> high_bit) & 1, 1)
            acc = acc + raised.astype(jnp.float32) * (pr * pr + pi * pi)
        return acc

    weight = lax.fori_loop(0, groups // 4, combine, zero)
    weight = total(jnp.where(set_low | far_jump, weight, 0.0))
    gain = jnp.sqrt((rows_total * LANES) / weight)

    def put(g, re, im):
        out[pl.ds(pl.multiple_of(g * 16, 16), 8, stride=2), :] = re
        out[pl.ds(g * 16 + 1, 8, stride=2), :] = im

    def stay(g, _):
        at = pl.ds(pl.multiple_of(g * 8, 8), 8)
        put(g, new_r[at, :], new_i[at, :])
        return 0

    def lower_far(g, _):
        at = pl.ds(pl.multiple_of((g ^ (1 << high_bit)) * 8, 8), 8)
        vacant = 1 - (((g ^ absolute) >> high_bit) & 1)
        factor = gain * vacant.astype(jnp.float32)
        put(g, factor * new_r[at, :], factor * new_i[at, :])
        return 0

    def lower_lane(g, _):
        at = pl.ds(pl.multiple_of(g * 8, 8), 8)
        shift = LANES - (1 << low_bit)
        factor = jnp.where(set_low, 0.0, gain)
        put(
            g,
            factor * pltpu.roll(new_r[at, :], shift, 1),
            factor * pltpu.roll(new_i[at, :], shift, 1),
        )
        return 0

    def lower_sublane(bit):
        def run(g, _):
            at = pl.ds(pl.multiple_of(g * 8, 8), 8)
            shift = 8 - (1 << bit)
            factor = jnp.where(set_low, 0.0, gain)
            put(
                g,
                factor * pltpu.roll(new_r[at, :], shift, 0),
                factor * pltpu.roll(new_i[at, :], shift, 0),
            )
            return 0

        return run

    def over_output(run):
        lax.fori_loop(0, groups_out, run, 0, unroll=4)

    pl.when(jump == spins)(lambda: over_output(stay))
    pl.when((jump >= 10) & (jump < spins))(lambda: over_output(lower_far))
    pl.when(jump < 7)(lambda: over_output(lower_lane))
    for bit in range(3):
        pl.when(jump == 7 + bit)(functools.partial(over_output, lower_sublane(bit)))


def body(amplitudes, couplings, fields, decays, channel):
    node_count = lax.axis_size("amp")
    high_bits = node_count.bit_length() - 1
    device = lax.axis_index("amp")
    local_len = amplitudes.shape[2]
    spins = fields.shape[0]
    rows_total = node_count * local_len // LANES
    groups = rows_total // 8
    pieces = gather_state(amplitudes, high_bits)

    smem = pl.BlockSpec(memory_space=pltpu.SMEM)
    vmem = pl.BlockSpec(memory_space=pltpu.VMEM)
    mats, low, row_table = pl.pallas_call(
        functools.partial(prepare, spins),
        out_shape=(
            jax.ShapeDtypeStruct((4, BLOCK, BLOCK), jnp.bfloat16),
            jax.ShapeDtypeStruct((32, LANES), jnp.float32),
            jax.ShapeDtypeStruct((8, groups), jnp.float32),
        ),
        in_specs=[smem] * 4,
        out_specs=(vmem, vmem, vmem),
        cost_estimate=pl.CostEstimate(flops=20_000_000, bytes_accessed=1_000_000, transcendentals=0),
        name="tables",
    )(couplings, fields, decays, (device * (local_len // LANES // 8)).reshape(1).astype(jnp.int32))
    result = pl.pallas_call(
        functools.partial(kernel, spins, [start for start, _ in pieces]),
        out_shape=jax.ShapeDtypeStruct((2 * local_len // LANES, LANES), jnp.float32),
        in_specs=[smem] * 4 + [vmem] * (2 + len(pieces)),
        out_specs=vmem,
        scratch_shapes=[
            pltpu.VMEM((KRYLOV, rows_total, LANES), jnp.float32),
            pltpu.VMEM((KRYLOV, rows_total, LANES), jnp.float32),
            pltpu.VMEM((rows_total, LANES), jnp.float32),
            pltpu.VMEM((rows_total, LANES), jnp.float32),
            pltpu.VMEM((rows_total, LANES), jnp.float32),
            pltpu.VMEM((rows_total, LANES), jnp.float32),
            pltpu.VMEM((2, rows_total // CHUNK, BLOCK, BLOCK), jnp.bfloat16),
            pltpu.VMEM((2, rows_total // CHUNK, BLOCK, BLOCK), jnp.bfloat16),
            pltpu.VMEM((LANES, LANES), jnp.float32),
            pltpu.VMEM((4,) + TILE, jnp.float32),
            pltpu.VMEM((KRYLOV,) + TILE, jnp.float32),
            pltpu.VMEM((KRYLOV * KRYLOV,) + TILE, jnp.float32),
            pltpu.VMEM((KRYLOV * KRYLOV,) + TILE, jnp.float32),
        ],
        compiler_params=pltpu.CompilerParams(vmem_limit_bytes=60 * 1024 * 1024),
        name="trajectory",
    )(
        fields,
        row_table,
        channel.reshape(1),
        device.reshape(1).astype(jnp.int32),
        low,
        mats,
        *[interleaved(piece) for _, piece in pieces],
    )
    rows = local_len // LANES
    return result.reshape(rows, 2, LANES).transpose(1, 0, 2).reshape(1, 2, local_len)


def solution(mesh):
    placed = (P("traj", None, "amp"), P(), P(), P(), P("traj"))
    return jax.shard_map(
        body, mesh=mesh, in_specs=placed, out_specs=P("traj", None, "amp"), check_vma=False
    )
```

```python
import functools
import jax
import jax.numpy as jnp
from jax import lax
from jax.experimental import pallas as pl
from jax.experimental.pallas import tpu as pltpu
from jax.sharding import PartitionSpec as P

KRYLOV = 8
time_step = 0.7
squarings = 8
taylor_order = 10
highest = lax.Precision.HIGHEST
LANES = 128
TILE = (8, LANES)
BLOCK = 256
CHUNK = 2 * BLOCK
SET_BITS = 2


def partner(value, mask):
    count = lax.axis_size("amp")
    return lax.ppermute(value, "amp", [(i, i ^ mask) for i in range(count)])


def gather_state(own, high_bits):
    rows = own.shape[2] // LANES
    if high_bits == 2:
        half = own.shape[2] // 2
        low, high = own[:, :, :half], own[:, :, half:]
        first_low, second_high = partner(low, 1), partner(high, 2)
        first_high, second_low = partner(high, 1), partner(low, 2)
        third_low, third_high = partner(first_low, 2), partner(second_high, 1)
        parts = [own, first_low, first_high, second_low, second_high, third_low, third_high]
        starts = [0, rows, rows + rows // 2, 2 * rows, 2 * rows + rows // 2, 3 * rows, 3 * rows + rows // 2]
        return list(zip(starts, parts))
    pieces = [(0, own)]
    for bit in range(high_bits):
        pieces += [(start + (rows << bit), partner(piece, 1 << bit)) for start, piece in pieces]
    return pieces


def interleaved(piece):
    rows = piece.shape[2] // LANES
    return piece.reshape(2, rows, LANES).transpose(1, 0, 2).reshape(2 * rows, LANES)


def splat(value):
    return jnp.broadcast_to(value, TILE)


def total(acc):
    return splat(jnp.sum(acc, keepdims=True))


def cmul(a, b):
    return (a[0] * b[0] - a[1] * b[1], a[0] * b[1] + a[1] * b[0])


def conj(a):
    return (a[0], -a[1])


def sub(a, b):
    return (a[0] - b[0], a[1] - b[1])


def scale(a, r):
    return (a[0] * r, a[1] * r)


def prepare(spins, couplings, fields, decays, device, mats, low, rows):
    tile_ids = lax.broadcasted_iota(jnp.int32, TILE, 0) * LANES + lax.broadcasted_iota(jnp.int32, TILE, 1)
    bits = [(tile_ids >> i & 1).astype(jnp.float32) for i in range(10)]
    signs = [1.0 - 2.0 * b for b in bits]
    real = -sum(couplings[i] * (signs[i] * signs[i + 1]) for i in range(9))
    bond = couplings[9] * signs[9]
    low[0:8, :] = real - bond
    low[8:16, :] = real + bond
    low[16:24, :] = -0.5 * sum(decays[i] * bits[i] for i in range(10))
    low[24:32, :] = jnp.zeros(TILE, jnp.float32)
    wide = rows.shape
    ids = lax.broadcasted_iota(jnp.int32, wide, 1) ^ device[0]
    bits = [(ids >> i & 1).astype(jnp.float32) for i in range(spins - 10)]
    signs = [1.0 - 2.0 * b for b in bits]
    real = -sum(couplings[10 + i] * (signs[i] * signs[i + 1]) for i in range(spins - 11))
    imag = -0.5 * sum(decays[10 + i] * bits[i] for i in range(spins - 10))
    rows[...] = jnp.where(lax.broadcasted_iota(jnp.int32, wide, 0) == 0, real, imag)
    for r in range(0, BLOCK, 32):
        shape = (32, BLOCK)
        crossed = (r + lax.broadcasted_iota(jnp.int32, shape, 0)) ^ lax.broadcasted_iota(jnp.int32, shape, 1)
        for side in range(2):
            m = jnp.zeros(shape, jnp.float32)
            for i in range(8):
                spin = 7 + i if side == 0 else (i if i < 7 else 15)
                m = jnp.where(crossed == 1 << i, -fields[spin], m)
            h = m.astype(jnp.bfloat16)
            mats[2 * side, r : r + 32, :] = h
            mats[2 * side + 1, r : r + 32, :] = (m - h.astype(jnp.float32)).astype(jnp.bfloat16)


def kernel(spins, starts, *refs):
    count = len(starts)
    fields, row_table, channel, device = refs[:4]
    low_table, mats = refs[4:6]
    pieces = refs[6 : 6 + count]
    out = refs[6 + count]
    basis_r, basis_i, cur_r, cur_i, new_r, new_i, high, low, table, coefs, norms, inner_r, inner_i, staged, arrived = refs[7 + count :]
    rows_total = new_r.shape[0]
    groups = rows_total // 8
    rows_out = out.shape[0] // 2
    zero = jnp.zeros(TILE, jnp.float32)
    dot = functools.partial(jnp.dot, preferred_element_type=jnp.float32)

    copies = []
    for i, (start, piece) in enumerate(zip(starts, pieces)):
        into = staged.at[pl.ds(2 * start, piece.shape[0]), :]
        copies.append(pltpu.make_async_copy(piece, into, arrived.at[i]))
        copies[-1].start()

    def clear(t, carry):
        at = pl.ds(pl.multiple_of(t * 8, 8), 8)
        for ref in (cur_r, cur_i, basis_r.at[0], basis_i.at[0]):
            ref[at, :] = zero
        return carry

    lax.fori_loop(0, groups, clear, 0, unroll=8)

    for start, piece, copy in zip(starts, pieces, copies):
        copy.wait()

        def take(g, carry, start=start):
            row = pl.multiple_of(start + g * 8, 8)
            new_r[pl.ds(row, 8), :] = staged[pl.ds(pl.multiple_of(2 * start + g * 16, 16), 8, stride=2), :]
            new_i[pl.ds(row, 8), :] = staged[pl.ds(2 * start + g * 16 + 1, 8, stride=2), :]
            return carry

        lax.fori_loop(0, piece.shape[0] // 16, take, 0, unroll=8)

    def block_flips(c):
        base = pl.multiple_of(c * CHUNK, CHUNK)
        both = mats[0:2].reshape(2 * BLOCK, BLOCK)
        for part, ref in ((0, new_r), (1, new_i)):
            xh, xl = high[part, c], low[part, c]
            z = dot(both, xh)
            y = z[:BLOCK] + z[BLOCK:] + dot(mats[0], xl)
            z = dot(jnp.concatenate([xh, xl]), mats[2])
            y = y + z[:BLOCK] + z[BLOCK:] + dot(xh, mats[3])
            ref[pl.ds(base, BLOCK), :] = y[:, :LANES]
            ref[pl.ds(base + BLOCK, BLOCK), :] = y[:, LANES:]

    def halves(part, c, block, r, value):
        h = value.astype(jnp.bfloat16)
        l = (value - h.astype(jnp.float32)).astype(jnp.bfloat16)
        high[part, c, pl.ds(r, 16), pl.ds(block * LANES, LANES)] = h
        low[part, c, pl.ds(r, 16), pl.ds(block * LANES, LANES)] = l

    near = [(b, fields[7 + b]) for b in range(9, 9 + SET_BITS)]
    far = [(b, fields[7 + b]) for b in range(9 + SET_BITS, spins - 7)]
    sets = 1 << SET_BITS
    span = CHUNK * sets
    ones = jnp.ones(TILE, jnp.float32)
    for i, value in enumerate((ones, zero, zero, zero)):
        coefs[i] = value

    def one_step(step):
        earlier = jnp.maximum(step - 2, 0)

        def make(t, acc):
            start = pl.multiple_of(t * span, span)
            sc, ar, ai, b = [jnp.concatenate([coefs[i], coefs[i]]) for i in range(4)]
            lr, li = (low_table[0:8, :], low_table[8:16, :]), low_table[16:24, :]

            def vector(i, acc):
                for block in range(2):
                    for r in range(0, BLOCK, 16):
                        at = pl.ds(start + i * CHUNK + block * BLOCK + r, 16)
                        pr, pi = cur_r[at, :], cur_i[at, :]
                        re = sc * new_r[at, :] - (ar * pr - ai * pi) - b * basis_r[earlier, at, :]
                        im = sc * new_i[at, :] - (ar * pi + ai * pr) - b * basis_i[earlier, at, :]
                        cur_r[at, :] = re
                        cur_i[at, :] = im
                        sq = re * re + im * im
                        acc = acc + (sq[:8] + sq[8:])
                        c = t * sets + i
                        halves(0, c, block, r, re)
                        halves(1, c, block, r, im)
                return acc

            def rest(i):
                for r in range(0, CHUNK, 8):
                    row = i * CHUNK + r
                    at = pl.ds(start + row, 8)
                    xr, xi = cur_r[at, :], cur_i[at, :]
                    wr, wi = new_r[at, :], new_i[at, :]
                    g = t * (span // 8) + row // 8
                    dr = lr[(r // 8) & 1] + row_table[0, g]
                    di = li + row_table[1, g]
                    wr = wr + (dr * xr - di * xi)
                    wi = wi + (dr * xi + di * xr)
                    for bit, weight in near:
                        other = pl.ds(start + (row ^ (1 << bit)), 8)
                        wr = wr - weight * cur_r[other, :]
                        wi = wi - weight * cur_i[other, :]
                    new_r[at, :] = wr
                    new_i[at, :] = wi

            for i in range(sets):
                acc = vector(i, acc)
                block_flips(t * sets + i)
            for i in range(sets):
                rest(i)
            return acc

        norms[step] = total(lax.fori_loop(0, rows_total // span, make, zero))

    def products(step):
        count_rows = 32 if step < 3 else 16

        def apply(t, accs):
            base = pl.multiple_of(t * (8 * count_rows), 8 * count_rows)
            at = [pl.ds(pl.multiple_of(base + 8 * r, 8), 8) for r in range(count_rows)]
            accs = list(accs)
            for first in range(0, count_rows, 4):
                w = []
                for r in range(first, first + 4):
                    wr, wi = new_r[at[r], :], new_i[at[r], :]
                    for bit, weight in far:
                        other = pl.ds(pl.multiple_of((base ^ (1 << bit)) + 8 * r, 8), 8)
                        wr = wr - weight * cur_r[other, :]
                        wi = wi - weight * cur_i[other, :]
                    if step + 1 < KRYLOV:
                        new_r[at[r], :] = wr
                        new_i[at[r], :] = wi
                    w.append((wr, wi, wr + wi))
                for k in range(step + 1):
                    found = []
                    for r in range(first, first + 4):
                        if k == step:
                            ur, ui = cur_r[at[r], :], cur_i[at[r], :]
                            basis_r[k, at[r], :] = ur
                            basis_i[k, at[r], :] = ui
                        else:
                            ur, ui = basis_r[k, at[r], :], basis_i[k, at[r], :]
                        wr, wi, ws = w[r - first]
                        found.append((ur * wr, ui * wi, (ur - ui) * ws))
                    for part in range(3):
                        x = [f[part] for f in found]
                        accs[3 * k + part] = accs[3 * k + part] + ((x[0] + x[1]) + (x[2] + x[3]))
            return tuple(accs)

        sums = lax.fori_loop(0, groups // count_rows, apply, (zero,) * (3 * step + 3))
        unit = lax.rsqrt(norms[0]) if step == 0 else ones
        found = []
        for k in range(step + 1):
            rr, ii, mixed = sums[3 * k : 3 * k + 3]
            found += [total(rr + ii) * unit, total(mixed - rr + ii) * unit]
        for k in range(step + 1):
            inner_r[step * KRYLOV + k] = found[2 * k]
            inner_i[step * KRYLOV + k] = found[2 * k + 1]
        inverse = 1.0 / norms[step]
        coefs[0] = unit
        coefs[1] = found[2 * step] * inverse
        coefs[2] = found[2 * step + 1] * inverse
        coefs[3] = found[2 * step - 2] / norms[step - 1] if step > 0 else zero

    @pl.loop(0, KRYLOV)
    def _(step):
        one_step(step)
        for s in range(KRYLOV):
            pl.when(step == s)(functools.partial(products, s))

    norm = [norms[j] for j in range(KRYLOV)]
    gram, diag_a, real_b = {(0, 0): (norm[0], zero)}, [], []
    read = lambda k, j: (inner_r[j * KRYLOV + k], inner_i[j * KRYLOV + k])
    g = lambda i, j: gram[i, j] if i <= j else conj(gram[j, i])
    for j in range(KRYLOV - 1):
        diag_a.append(scale(read(j, j), 1.0 / norm[j]))
        real_b.append(read(j - 1, j)[0] / norm[j - 1] if j > 0 else zero)
        for k in range(j + 1):
            value = sub(read(k, j), cmul(diag_a[j], g(k, j)))
            if j > 0:
                value = sub(value, scale(g(k, j - 1), real_b[j]))
            gram[k, j + 1] = value
        gram[j + 1, j + 1] = (norm[j + 1], zero)
    inner = [read(k, KRYLOV - 1) for k in range(KRYLOV)]

    size = [jnp.sqrt(x) for x in norm]
    inv = [1.0 / x for x in size]
    mat = {}
    for j in range(KRYLOV):
        for k in range(j + 1):
            mat[j, k] = conj(scale(gram[k, j], inv[k] * inv[j]))
    rhs = [scale(inner[k], inv[k] * inv[KRYLOV - 1]) for k in range(KRYLOV)]
    factor, pivot = {}, []
    for j in range(KRYLOV):
        d = mat[j, j][0]
        for k in range(j):
            d = d - (factor[j, k][0] * factor[j, k][0] + factor[j, k][1] * factor[j, k][1]) * pivot[k]
        pivot.append(d)
        r = 1.0 / d
        for i in range(j + 1, KRYLOV):
            x = mat[i, j]
            for k in range(j):
                x = sub(x, scale(cmul(factor[i, k], conj(factor[j, k])), pivot[k]))
            factor[i, j] = scale(x, r)
    last = list(rhs)
    for i in range(KRYLOV):
        for k in range(i):
            last[i] = sub(last[i], cmul(factor[i, k], last[k]))
    last = [scale(x, 1.0 / pivot[i]) for i, x in enumerate(last)]
    for i in reversed(range(KRYLOV)):
        for k in range(i + 1, KRYLOV):
            last[i] = sub(last[i], cmul(conj(factor[k, i]), last[k]))

    entries = {}
    for j in range(KRYLOV - 1):
        entries[j, j] = diag_a[j] if j > 0 else scale(diag_a[0], size[0])
        grow = size[1] if j == 0 else size[j + 1] * inv[j]
        entries[j + 1, j] = (grow, zero)
        if j > 0:
            entries[j - 1, j] = (real_b[j] * (size[j - 1] * inv[j]), zero)
    for i in range(KRYLOV):
        entries[i, KRYLOV - 1] = last[i]
    order = 2 * KRYLOV
    code = lax.broadcasted_iota(jnp.int32, TILE, 0) * LANES + lax.broadcasted_iota(jnp.int32, TILE, 1)
    quads = [[zero, zero], [zero, zero]]
    for (i, j), (re, im) in entries.items():
        here = code == i * LANES + j
        there = code == i * LANES + j + KRYLOV
        ar, ai = time_step * im, -time_step * re
        quads[0][0] = jnp.where(here, ar, jnp.where(there, -ai, quads[0][0]))
        quads[1][0] = jnp.where(here, ai, jnp.where(there, ar, quads[1][0]))
    table[...] = jnp.zeros_like(table)
    table[0:8, :] = quads[0][0] * (1.0 / 2.0**squarings)
    table[8:16, :] = quads[1][0] * (1.0 / 2.0**squarings)
    one = table[0:order, :]
    eye = jnp.where(
        lax.broadcasted_iota(jnp.int32, one.shape, 0) == lax.broadcasted_iota(jnp.int32, one.shape, 1), 1.0, 0.0
    )
    fill = jnp.zeros((LANES - order, LANES), jnp.float32)

    def times(a, b):
        return dot(a, jnp.concatenate([b, fill]), precision=highest)

    two = times(one, one)
    three = times(two, one)
    f = [1.0]
    for d in range(1, taylor_order + 1):
        f.append(f[-1] / d)
    series = f[9] * eye + f[10] * one
    for d in (6, 3, 0):
        series = (f[d] * eye + f[d + 1] * one + f[d + 2] * two) + times(three, series)
    for repeat in range(squarings):
        series = times(series, series)
    table[0:order, :] = series
    weights = []
    for k in range(KRYLOV):
        c = size[0] * inv[k]
        cr, ci = splat(table[k : k + 1, 0:1]) * c, splat(table[k + 8 : k + 9, 0:1]) * c
        weights.append((cr, ci - cr, cr + ci))

    jump = channel[0]
    first = device[0]
    lane = lax.broadcasted_iota(jnp.int32, TILE, 1)
    sublane = lax.broadcasted_iota(jnp.int32, TILE, 0)
    inside = sublane * LANES + lane
    far_jump = jump >= 10
    low_bit = jnp.where(far_jump, 0, jump)
    high_bit = jnp.where(far_jump, jump - 10, 0)
    set_low = ((inside >> low_bit) & 1) == 1
    groups_out = rows_out // 8
    absolute = first * groups_out

    def combine(c, acc):
        for r in range(4):
            g = c * 4 + r
            at = pl.ds(pl.multiple_of(g * 8, 8), 8)
            s1, s2, s3 = zero, zero, zero
            for k in range(KRYLOV):
                cr, less, more = weights[k]
                ur, ui = basis_r[k, at, :], basis_i[k, at, :]
                s1 = s1 + cr * (ur + ui)
                s2 = s2 + less * ur
                s3 = s3 + more * ui
            pr, pi = s1 - s3, s1 + s2
            new_r[at, :] = pr
            new_i[at, :] = pi
            raised = jnp.where(far_jump, ((g ^ absolute) >> high_bit) & 1, 1)
            acc = acc + raised.astype(jnp.float32) * (pr * pr + pi * pi)
        return acc

    weight = lax.fori_loop(0, groups // 4, combine, zero)
    weight = total(jnp.where(set_low | far_jump, weight, 0.0))
    gain = jnp.sqrt((rows_total * LANES) / weight)

    def put(g, re, im):
        out[pl.ds(pl.multiple_of(g * 16, 16), 8, stride=2), :] = re
        out[pl.ds(g * 16 + 1, 8, stride=2), :] = im

    def stay(g, _):
        at = pl.ds(pl.multiple_of(g * 8, 8), 8)
        put(g, new_r[at, :], new_i[at, :])
        return 0

    def lower_far(g, _):
        at = pl.ds(pl.multiple_of((g ^ (1 << high_bit)) * 8, 8), 8)
        vacant = 1 - (((g ^ absolute) >> high_bit) & 1)
        factor = gain * vacant.astype(jnp.float32)
        put(g, factor * new_r[at, :], factor * new_i[at, :])
        return 0

    def lower_lane(g, _):
        at = pl.ds(pl.multiple_of(g * 8, 8), 8)
        shift = LANES - (1 << low_bit)
        factor = jnp.where(set_low, 0.0, gain)
        put(
            g,
            factor * pltpu.roll(new_r[at, :], shift, 1),
            factor * pltpu.roll(new_i[at, :], shift, 1),
        )
        return 0

    def lower_sublane(bit):
        def run(g, _):
            at = pl.ds(pl.multiple_of(g * 8, 8), 8)
            shift = 8 - (1 << bit)
            factor = jnp.where(set_low, 0.0, gain)
            put(
                g,
                factor * pltpu.roll(new_r[at, :], shift, 0),
                factor * pltpu.roll(new_i[at, :], shift, 0),
            )
            return 0

        return run

    def over_output(run):
        lax.fori_loop(0, groups_out, run, 0, unroll=4)

    pl.when(jump == spins)(lambda: over_output(stay))
    pl.when((jump >= 10) & (jump < spins))(lambda: over_output(lower_far))
    pl.when(jump < 7)(lambda: over_output(lower_lane))
    for bit in range(3):
        pl.when(jump == 7 + bit)(functools.partial(over_output, lower_sublane(bit)))


def body(amplitudes, couplings, fields, decays, channel):
    node_count = lax.axis_size("amp")
    high_bits = node_count.bit_length() - 1
    device = lax.axis_index("amp")
    local_len = amplitudes.shape[2]
    spins = fields.shape[0]
    rows_total = node_count * local_len // LANES
    groups = rows_total // 8
    pieces = gather_state(amplitudes, high_bits)

    smem = pl.BlockSpec(memory_space=pltpu.SMEM)
    vmem = pl.BlockSpec(memory_space=pltpu.VMEM)
    mats, low, row_table = pl.pallas_call(
        functools.partial(prepare, spins),
        out_shape=(
            jax.ShapeDtypeStruct((4, BLOCK, BLOCK), jnp.bfloat16),
            jax.ShapeDtypeStruct((32, LANES), jnp.float32),
            jax.ShapeDtypeStruct((8, groups), jnp.float32),
        ),
        in_specs=[smem] * 4,
        out_specs=(vmem, vmem, vmem),
        cost_estimate=pl.CostEstimate(flops=20_000_000, bytes_accessed=1_000_000, transcendentals=0),
        name="tables",
    )(couplings, fields, decays, (device * (local_len // LANES // 8)).reshape(1).astype(jnp.int32))
    result = pl.pallas_call(
        functools.partial(kernel, spins, [start for start, _ in pieces]),
        out_shape=jax.ShapeDtypeStruct((2 * local_len // LANES, LANES), jnp.float32),
        in_specs=[smem] * 4 + [vmem] * 2 + [pl.BlockSpec(memory_space=pl.ANY)] * len(pieces),
        out_specs=vmem,
        scratch_shapes=[
            pltpu.VMEM((KRYLOV, rows_total, LANES), jnp.float32),
            pltpu.VMEM((KRYLOV, rows_total, LANES), jnp.float32),
            pltpu.VMEM((rows_total, LANES), jnp.float32),
            pltpu.VMEM((rows_total, LANES), jnp.float32),
            pltpu.VMEM((rows_total, LANES), jnp.float32),
            pltpu.VMEM((rows_total, LANES), jnp.float32),
            pltpu.VMEM((2, rows_total // CHUNK, BLOCK, BLOCK), jnp.bfloat16),
            pltpu.VMEM((2, rows_total // CHUNK, BLOCK, BLOCK), jnp.bfloat16),
            pltpu.VMEM((LANES, LANES), jnp.float32),
            pltpu.VMEM((4,) + TILE, jnp.float32),
            pltpu.VMEM((KRYLOV,) + TILE, jnp.float32),
            pltpu.VMEM((KRYLOV * KRYLOV,) + TILE, jnp.float32),
            pltpu.VMEM((KRYLOV * KRYLOV,) + TILE, jnp.float32),
            pltpu.VMEM((2 * rows_total, LANES), jnp.float32),
            pltpu.SemaphoreType.DMA((len(pieces),)),
        ],
        compiler_params=pltpu.CompilerParams(vmem_limit_bytes=60 * 1024 * 1024),
        name="trajectory",
    )(
        fields,
        row_table,
        channel.reshape(1),
        device.reshape(1).astype(jnp.int32),
        low,
        mats,
        *[interleaved(piece) for _, piece in pieces],
    )
    rows = local_len // LANES
    return result.reshape(rows, 2, LANES).transpose(1, 0, 2).reshape(1, 2, local_len)


def solution(mesh):
    placed = (P("traj", None, "amp"), P(), P(), P(), P("traj"))
    return jax.shard_map(
        body, mesh=mesh, in_specs=placed, out_specs=P("traj", None, "amp"), check_vma=False
    )
```

```python
import functools
import jax
import jax.numpy as jnp
from jax import lax
from jax.experimental import pallas as pl
from jax.experimental.pallas import tpu as pltpu
from jax.sharding import PartitionSpec as P

KRYLOV = 8
time_step = 0.7
squarings = 8
taylor_order = 10
highest = lax.Precision.HIGHEST
LANES = 128
TILE = (8, LANES)
BLOCK = 256
CHUNK = 2 * BLOCK
SET_BITS = 3


def partner(value, mask):
    count = lax.axis_size("amp")
    return lax.ppermute(value, "amp", [(i, i ^ mask) for i in range(count)])


def gather_state(own, high_bits):
    rows = own.shape[2] // LANES
    if high_bits == 2:
        half = own.shape[2] // 2
        low, high = own[:, :, :half], own[:, :, half:]
        first_low, second_high = partner(low, 1), partner(high, 2)
        first_high, second_low = partner(high, 1), partner(low, 2)
        third_low, third_high = partner(first_low, 2), partner(second_high, 1)
        parts = [own, first_low, first_high, second_low, second_high, third_low, third_high]
        starts = [0, rows, rows + rows // 2, 2 * rows, 2 * rows + rows // 2, 3 * rows, 3 * rows + rows // 2]
        return list(zip(starts, parts))
    pieces = [(0, own)]
    for bit in range(high_bits):
        pieces += [(start + (rows << bit), partner(piece, 1 << bit)) for start, piece in pieces]
    return pieces


def interleaved(piece):
    rows = piece.shape[2] // LANES
    return piece.reshape(2, rows, LANES).transpose(1, 0, 2).reshape(2 * rows, LANES)


def splat(value):
    return jnp.broadcast_to(value, TILE)


def total(acc):
    return splat(jnp.sum(acc, keepdims=True))


def cmul(a, b):
    return (a[0] * b[0] - a[1] * b[1], a[0] * b[1] + a[1] * b[0])


def conj(a):
    return (a[0], -a[1])


def sub(a, b):
    return (a[0] - b[0], a[1] - b[1])


def scale(a, r):
    return (a[0] * r, a[1] * r)


def prepare(spins, couplings, fields, decays, device, mats, low, rows):
    tile_ids = lax.broadcasted_iota(jnp.int32, TILE, 0) * LANES + lax.broadcasted_iota(jnp.int32, TILE, 1)
    bits = [(tile_ids >> i & 1).astype(jnp.float32) for i in range(10)]
    signs = [1.0 - 2.0 * b for b in bits]
    real = -sum(couplings[i] * (signs[i] * signs[i + 1]) for i in range(9))
    bond = couplings[9] * signs[9]
    low[0:8, :] = real - bond
    low[8:16, :] = real + bond
    low[16:24, :] = -0.5 * sum(decays[i] * bits[i] for i in range(10))
    low[24:32, :] = jnp.zeros(TILE, jnp.float32)
    wide = rows.shape
    ids = lax.broadcasted_iota(jnp.int32, wide, 1) ^ device[0]
    bits = [(ids >> i & 1).astype(jnp.float32) for i in range(spins - 10)]
    signs = [1.0 - 2.0 * b for b in bits]
    real = -sum(couplings[10 + i] * (signs[i] * signs[i + 1]) for i in range(spins - 11))
    imag = -0.5 * sum(decays[10 + i] * bits[i] for i in range(spins - 10))
    rows[...] = jnp.where(lax.broadcasted_iota(jnp.int32, wide, 0) == 0, real, imag)
    for r in range(0, BLOCK, 32):
        shape = (32, BLOCK)
        crossed = (r + lax.broadcasted_iota(jnp.int32, shape, 0)) ^ lax.broadcasted_iota(jnp.int32, shape, 1)
        for side in range(2):
            m = jnp.zeros(shape, jnp.float32)
            for i in range(8):
                spin = 7 + i if side == 0 else (i if i < 7 else 15)
                m = jnp.where(crossed == 1 << i, -fields[spin], m)
            h = m.astype(jnp.bfloat16)
            mats[2 * side, r : r + 32, :] = h
            mats[2 * side + 1, r : r + 32, :] = (m - h.astype(jnp.float32)).astype(jnp.bfloat16)


def kernel(spins, starts, *refs):
    count = len(starts)
    fields, row_table, channel, device = refs[:4]
    low_table, mats = refs[4:6]
    pieces = refs[6 : 6 + count]
    out = refs[6 + count]
    basis_r, basis_i, cur_r, cur_i, new_r, new_i, high, low, table, coefs, norms, inner_r, inner_i, staged, arrived = refs[7 + count :]
    rows_total = new_r.shape[0]
    groups = rows_total // 8
    rows_out = out.shape[0] // 2
    zero = jnp.zeros(TILE, jnp.float32)
    dot = functools.partial(jnp.dot, preferred_element_type=jnp.float32)

    copies = []
    for i, (start, piece) in enumerate(zip(starts, pieces)):
        into = staged.at[pl.ds(2 * start, piece.shape[0]), :]
        copies.append(pltpu.make_async_copy(piece, into, arrived.at[i]))
        copies[-1].start()

    def clear(t, carry):
        at = pl.ds(pl.multiple_of(t * 8, 8), 8)
        for ref in (cur_r, cur_i, basis_r.at[0], basis_i.at[0]):
            ref[at, :] = zero
        return carry

    lax.fori_loop(0, groups, clear, 0, unroll=8)

    for start, piece, copy in zip(starts, pieces, copies):
        copy.wait()

        def take(g, carry, start=start):
            row = pl.multiple_of(start + g * 8, 8)
            new_r[pl.ds(row, 8), :] = staged[pl.ds(pl.multiple_of(2 * start + g * 16, 16), 8, stride=2), :]
            new_i[pl.ds(row, 8), :] = staged[pl.ds(2 * start + g * 16 + 1, 8, stride=2), :]
            return carry

        lax.fori_loop(0, piece.shape[0] // 16, take, 0, unroll=8)

    def block_flips(c):
        base = pl.multiple_of(c * CHUNK, CHUNK)
        both = mats[0:2].reshape(2 * BLOCK, BLOCK)
        for part, ref in ((0, new_r), (1, new_i)):
            xh, xl = high[part, c], low[part, c]
            z = dot(both, xh)
            y = z[:BLOCK] + z[BLOCK:] + dot(mats[0], xl)
            z = dot(jnp.concatenate([xh, xl]), mats[2])
            y = y + z[:BLOCK] + z[BLOCK:] + dot(xh, mats[3])
            ref[pl.ds(base, BLOCK), :] = y[:, :LANES]
            ref[pl.ds(base + BLOCK, BLOCK), :] = y[:, LANES:]

    def halves(part, c, block, r, value):
        h = value.astype(jnp.bfloat16)
        l = (value - h.astype(jnp.float32)).astype(jnp.bfloat16)
        high[part, c, pl.ds(r, 16), pl.ds(block * LANES, LANES)] = h
        low[part, c, pl.ds(r, 16), pl.ds(block * LANES, LANES)] = l

    near = [(b, fields[7 + b]) for b in range(9, 9 + SET_BITS)]
    far = [(b, fields[7 + b]) for b in range(9 + SET_BITS, spins - 7)]
    sets = 1 << SET_BITS
    span = CHUNK * sets
    ones = jnp.ones(TILE, jnp.float32)
    for i, value in enumerate((ones, zero, zero, zero)):
        coefs[i] = value

    def one_step(step):
        earlier = jnp.maximum(step - 2, 0)

        def make(t, acc):
            start = pl.multiple_of(t * span, span)
            sc, ar, ai, b = [jnp.concatenate([coefs[i], coefs[i]]) for i in range(4)]
            lr, li = (low_table[0:8, :], low_table[8:16, :]), low_table[16:24, :]

            def vector(i, acc):
                for block in range(2):
                    for r in range(0, BLOCK, 16):
                        at = pl.ds(start + i * CHUNK + block * BLOCK + r, 16)
                        pr, pi = cur_r[at, :], cur_i[at, :]
                        re = sc * new_r[at, :] - (ar * pr - ai * pi) - b * basis_r[earlier, at, :]
                        im = sc * new_i[at, :] - (ar * pi + ai * pr) - b * basis_i[earlier, at, :]
                        cur_r[at, :] = re
                        cur_i[at, :] = im
                        sq = re * re + im * im
                        acc = acc + (sq[:8] + sq[8:])
                        c = t * sets + i
                        halves(0, c, block, r, re)
                        halves(1, c, block, r, im)
                return acc

            def rest(i):
                for r in range(0, CHUNK, 8):
                    row = i * CHUNK + r
                    at = pl.ds(start + row, 8)
                    xr, xi = cur_r[at, :], cur_i[at, :]
                    wr, wi = new_r[at, :], new_i[at, :]
                    g = t * (span // 8) + row // 8
                    dr = lr[(r // 8) & 1] + row_table[0, g]
                    di = li + row_table[1, g]
                    wr = wr + (dr * xr - di * xi)
                    wi = wi + (dr * xi + di * xr)
                    for bit, weight in near:
                        other = pl.ds(start + (row ^ (1 << bit)), 8)
                        wr = wr - weight * cur_r[other, :]
                        wi = wi - weight * cur_i[other, :]
                    new_r[at, :] = wr
                    new_i[at, :] = wi

            for i in range(sets):
                acc = vector(i, acc)
                block_flips(t * sets + i)
            for i in range(sets):
                rest(i)
            return acc

        norms[step] = total(lax.fori_loop(0, rows_total // span, make, zero))

    def products(step):
        count_rows = 32 if step < 3 else 16

        def apply(t, accs):
            base = pl.multiple_of(t * (8 * count_rows), 8 * count_rows)
            at = [pl.ds(pl.multiple_of(base + 8 * r, 8), 8) for r in range(count_rows)]
            accs = list(accs)
            for first in range(0, count_rows, 4):
                w = []
                for r in range(first, first + 4):
                    wr, wi = new_r[at[r], :], new_i[at[r], :]
                    for bit, weight in far:
                        other = pl.ds(pl.multiple_of((base ^ (1 << bit)) + 8 * r, 8), 8)
                        wr = wr - weight * cur_r[other, :]
                        wi = wi - weight * cur_i[other, :]
                    if step + 1 < KRYLOV:
                        new_r[at[r], :] = wr
                        new_i[at[r], :] = wi
                    w.append((wr, wi, wr + wi))
                for k in range(step + 1):
                    found = []
                    for r in range(first, first + 4):
                        if k == step:
                            ur, ui = cur_r[at[r], :], cur_i[at[r], :]
                            basis_r[k, at[r], :] = ur
                            basis_i[k, at[r], :] = ui
                        else:
                            ur, ui = basis_r[k, at[r], :], basis_i[k, at[r], :]
                        wr, wi, ws = w[r - first]
                        found.append((ur * wr, ui * wi, (ur - ui) * ws))
                    for part in range(3):
                        x = [f[part] for f in found]
                        accs[3 * k + part] = accs[3 * k + part] + ((x[0] + x[1]) + (x[2] + x[3]))
            return tuple(accs)

        sums = lax.fori_loop(0, groups // count_rows, apply, (zero,) * (3 * step + 3))
        unit = lax.rsqrt(norms[0]) if step == 0 else ones
        found = []
        for k in range(step + 1):
            rr, ii, mixed = sums[3 * k : 3 * k + 3]
            found += [total(rr + ii) * unit, total(mixed - rr + ii) * unit]
        for k in range(step + 1):
            inner_r[step * KRYLOV + k] = found[2 * k]
            inner_i[step * KRYLOV + k] = found[2 * k + 1]
        inverse = 1.0 / norms[step]
        coefs[0] = unit
        coefs[1] = found[2 * step] * inverse
        coefs[2] = found[2 * step + 1] * inverse
        coefs[3] = found[2 * step - 2] / norms[step - 1] if step > 0 else zero

    @pl.loop(0, KRYLOV)
    def _(step):
        one_step(step)
        for s in range(KRYLOV):
            pl.when(step == s)(functools.partial(products, s))

    norm = [norms[j] for j in range(KRYLOV)]
    gram, diag_a, real_b = {(0, 0): (norm[0], zero)}, [], []
    read = lambda k, j: (inner_r[j * KRYLOV + k], inner_i[j * KRYLOV + k])
    g = lambda i, j: gram[i, j] if i <= j else conj(gram[j, i])
    for j in range(KRYLOV - 1):
        diag_a.append(scale(read(j, j), 1.0 / norm[j]))
        real_b.append(read(j - 1, j)[0] / norm[j - 1] if j > 0 else zero)
        for k in range(j + 1):
            value = sub(read(k, j), cmul(diag_a[j], g(k, j)))
            if j > 0:
                value = sub(value, scale(g(k, j - 1), real_b[j]))
            gram[k, j + 1] = value
        gram[j + 1, j + 1] = (norm[j + 1], zero)
    inner = [read(k, KRYLOV - 1) for k in range(KRYLOV)]

    size = [jnp.sqrt(x) for x in norm]
    inv = [1.0 / x for x in size]
    mat = {}
    for j in range(KRYLOV):
        for k in range(j + 1):
            mat[j, k] = conj(scale(gram[k, j], inv[k] * inv[j]))
    rhs = [scale(inner[k], inv[k] * inv[KRYLOV - 1]) for k in range(KRYLOV)]
    factor, pivot = {}, []
    for j in range(KRYLOV):
        d = mat[j, j][0]
        for k in range(j):
            d = d - (factor[j, k][0] * factor[j, k][0] + factor[j, k][1] * factor[j, k][1]) * pivot[k]
        pivot.append(d)
        r = 1.0 / d
        for i in range(j + 1, KRYLOV):
            x = mat[i, j]
            for k in range(j):
                x = sub(x, scale(cmul(factor[i, k], conj(factor[j, k])), pivot[k]))
            factor[i, j] = scale(x, r)
    last = list(rhs)
    for i in range(KRYLOV):
        for k in range(i):
            last[i] = sub(last[i], cmul(factor[i, k], last[k]))
    last = [scale(x, 1.0 / pivot[i]) for i, x in enumerate(last)]
    for i in reversed(range(KRYLOV)):
        for k in range(i + 1, KRYLOV):
            last[i] = sub(last[i], cmul(conj(factor[k, i]), last[k]))

    entries = {}
    for j in range(KRYLOV - 1):
        entries[j, j] = diag_a[j] if j > 0 else scale(diag_a[0], size[0])
        grow = size[1] if j == 0 else size[j + 1] * inv[j]
        entries[j + 1, j] = (grow, zero)
        if j > 0:
            entries[j - 1, j] = (real_b[j] * (size[j - 1] * inv[j]), zero)
    for i in range(KRYLOV):
        entries[i, KRYLOV - 1] = last[i]
    order = 2 * KRYLOV
    code = lax.broadcasted_iota(jnp.int32, TILE, 0) * LANES + lax.broadcasted_iota(jnp.int32, TILE, 1)
    quads = [[zero, zero], [zero, zero]]
    for (i, j), (re, im) in entries.items():
        here = code == i * LANES + j
        there = code == i * LANES + j + KRYLOV
        ar, ai = time_step * im, -time_step * re
        quads[0][0] = jnp.where(here, ar, jnp.where(there, -ai, quads[0][0]))
        quads[1][0] = jnp.where(here, ai, jnp.where(there, ar, quads[1][0]))
    table[...] = jnp.zeros_like(table)
    table[0:8, :] = quads[0][0] * (1.0 / 2.0**squarings)
    table[8:16, :] = quads[1][0] * (1.0 / 2.0**squarings)
    one = table[0:order, :]
    eye = jnp.where(
        lax.broadcasted_iota(jnp.int32, one.shape, 0) == lax.broadcasted_iota(jnp.int32, one.shape, 1), 1.0, 0.0
    )
    fill = jnp.zeros((LANES - order, LANES), jnp.float32)

    def times(a, b):
        return dot(a, jnp.concatenate([b, fill]), precision=highest)

    two = times(one, one)
    three = times(two, one)
    f = [1.0]
    for d in range(1, taylor_order + 1):
        f.append(f[-1] / d)
    series = f[9] * eye + f[10] * one
    for d in (6, 3, 0):
        series = (f[d] * eye + f[d + 1] * one + f[d + 2] * two) + times(three, series)
    for repeat in range(squarings):
        series = times(series, series)
    table[0:order, :] = series
    weights = []
    for k in range(KRYLOV):
        c = size[0] * inv[k]
        cr, ci = splat(table[k : k + 1, 0:1]) * c, splat(table[k + 8 : k + 9, 0:1]) * c
        weights.append((cr, ci - cr, cr + ci))

    jump = channel[0]
    first = device[0]
    lane = lax.broadcasted_iota(jnp.int32, TILE, 1)
    sublane = lax.broadcasted_iota(jnp.int32, TILE, 0)
    inside = sublane * LANES + lane
    far_jump = jump >= 10
    low_bit = jnp.where(far_jump, 0, jump)
    high_bit = jnp.where(far_jump, jump - 10, 0)
    set_low = ((inside >> low_bit) & 1) == 1
    groups_out = rows_out // 8
    absolute = first * groups_out

    def combine(c, acc):
        for r in range(4):
            g = c * 4 + r
            at = pl.ds(pl.multiple_of(g * 8, 8), 8)
            s1, s2, s3 = zero, zero, zero
            for k in range(KRYLOV):
                cr, less, more = weights[k]
                ur, ui = basis_r[k, at, :], basis_i[k, at, :]
                s1 = s1 + cr * (ur + ui)
                s2 = s2 + less * ur
                s3 = s3 + more * ui
            pr, pi = s1 - s3, s1 + s2
            new_r[at, :] = pr
            new_i[at, :] = pi
            raised = jnp.where(far_jump, ((g ^ absolute) >> high_bit) & 1, 1)
            acc = acc + raised.astype(jnp.float32) * (pr * pr + pi * pi)
        return acc

    weight = lax.fori_loop(0, groups // 4, combine, zero)
    weight = total(jnp.where(set_low | far_jump, weight, 0.0))
    gain = jnp.sqrt((rows_total * LANES) / weight)

    def put(g, re, im):
        out[pl.ds(pl.multiple_of(g * 16, 16), 8, stride=2), :] = re
        out[pl.ds(g * 16 + 1, 8, stride=2), :] = im

    def stay(g, _):
        at = pl.ds(pl.multiple_of(g * 8, 8), 8)
        put(g, new_r[at, :], new_i[at, :])
        return 0

    def lower_far(g, _):
        at = pl.ds(pl.multiple_of((g ^ (1 << high_bit)) * 8, 8), 8)
        vacant = 1 - (((g ^ absolute) >> high_bit) & 1)
        factor = gain * vacant.astype(jnp.float32)
        put(g, factor * new_r[at, :], factor * new_i[at, :])
        return 0

    def lower_lane(g, _):
        at = pl.ds(pl.multiple_of(g * 8, 8), 8)
        shift = LANES - (1 << low_bit)
        factor = jnp.where(set_low, 0.0, gain)
        put(
            g,
            factor * pltpu.roll(new_r[at, :], shift, 1),
            factor * pltpu.roll(new_i[at, :], shift, 1),
        )
        return 0

    def lower_sublane(bit):
        def run(g, _):
            at = pl.ds(pl.multiple_of(g * 8, 8), 8)
            shift = 8 - (1 << bit)
            factor = jnp.where(set_low, 0.0, gain)
            put(
                g,
                factor * pltpu.roll(new_r[at, :], shift, 0),
                factor * pltpu.roll(new_i[at, :], shift, 0),
            )
            return 0

        return run

    def over_output(run):
        lax.fori_loop(0, groups_out, run, 0, unroll=4)

    pl.when(jump == spins)(lambda: over_output(stay))
    pl.when((jump >= 10) & (jump < spins))(lambda: over_output(lower_far))
    pl.when(jump < 7)(lambda: over_output(lower_lane))
    for bit in range(3):
        pl.when(jump == 7 + bit)(functools.partial(over_output, lower_sublane(bit)))


def body(amplitudes, couplings, fields, decays, channel):
    node_count = lax.axis_size("amp")
    high_bits = node_count.bit_length() - 1
    device = lax.axis_index("amp")
    local_len = amplitudes.shape[2]
    spins = fields.shape[0]
    rows_total = node_count * local_len // LANES
    groups = rows_total // 8
    pieces = gather_state(amplitudes, high_bits)

    smem = pl.BlockSpec(memory_space=pltpu.SMEM)
    vmem = pl.BlockSpec(memory_space=pltpu.VMEM)
    mats, low, row_table = pl.pallas_call(
        functools.partial(prepare, spins),
        out_shape=(
            jax.ShapeDtypeStruct((4, BLOCK, BLOCK), jnp.bfloat16),
            jax.ShapeDtypeStruct((32, LANES), jnp.float32),
            jax.ShapeDtypeStruct((8, groups), jnp.float32),
        ),
        in_specs=[smem] * 4,
        out_specs=(vmem, vmem, vmem),
        cost_estimate=pl.CostEstimate(flops=20_000_000, bytes_accessed=1_000_000, transcendentals=0),
        name="tables",
    )(couplings, fields, decays, (device * (local_len // LANES // 8)).reshape(1).astype(jnp.int32))
    result = pl.pallas_call(
        functools.partial(kernel, spins, [start for start, _ in pieces]),
        out_shape=jax.ShapeDtypeStruct((2 * local_len // LANES, LANES), jnp.float32),
        in_specs=[smem] * 4 + [vmem] * 2 + [pl.BlockSpec(memory_space=pl.ANY)] * len(pieces),
        out_specs=vmem,
        scratch_shapes=[
            pltpu.VMEM((KRYLOV, rows_total, LANES), jnp.float32),
            pltpu.VMEM((KRYLOV, rows_total, LANES), jnp.float32),
            pltpu.VMEM((rows_total, LANES), jnp.float32),
            pltpu.VMEM((rows_total, LANES), jnp.float32),
            pltpu.VMEM((rows_total, LANES), jnp.float32),
            pltpu.VMEM((rows_total, LANES), jnp.float32),
            pltpu.VMEM((2, rows_total // CHUNK, BLOCK, BLOCK), jnp.bfloat16),
            pltpu.VMEM((2, rows_total // CHUNK, BLOCK, BLOCK), jnp.bfloat16),
            pltpu.VMEM((LANES, LANES), jnp.float32),
            pltpu.VMEM((4,) + TILE, jnp.float32),
            pltpu.VMEM((KRYLOV,) + TILE, jnp.float32),
            pltpu.VMEM((KRYLOV * KRYLOV,) + TILE, jnp.float32),
            pltpu.VMEM((KRYLOV * KRYLOV,) + TILE, jnp.float32),
            pltpu.VMEM((2 * rows_total, LANES), jnp.float32),
            pltpu.SemaphoreType.DMA((len(pieces),)),
        ],
        compiler_params=pltpu.CompilerParams(vmem_limit_bytes=60 * 1024 * 1024),
        name="trajectory",
    )(
        fields,
        row_table,
        channel.reshape(1),
        device.reshape(1).astype(jnp.int32),
        low,
        mats,
        *[interleaved(piece) for _, piece in pieces],
    )
    rows = local_len // LANES
    return result.reshape(rows, 2, LANES).transpose(1, 0, 2).reshape(1, 2, local_len)


def solution(mesh):
    placed = (P("traj", None, "amp"), P(), P(), P(), P("traj"))
    return jax.shard_map(
        body, mesh=mesh, in_specs=placed, out_specs=P("traj", None, "amp"), check_vma=False
    )
```
